32 devices in a mesh: dp: 4 (over y, x), expert: 4 (over z), mp: 2 (over core).
Axes of the slice: x: 2, y: 2, z: 4, core: 2. Of those that a mesh axis runs over, the one named last changes fastest.
Arguments:
- base_weights: bfloat16 [8, 2560, 3072], P('expert', None, 'mp'), may hold values from -6 to 6
- delta_blocks: bfloat16 [512, 128, 128], P(('dp', 'expert', 'mp')), may hold values from -4 to 4
- block_ids: int32 [512], P(('dp', 'expert', 'mp')), may hold values from 0 to 3839, as said below
- block_counts: int32 [256], P(('dp', 'expert', 'mp')), may hold values from 0 to 2, as said below
- owner_map: int32 [8], replicated, may hold values from 0 to 7, as said below
Outputs:
- merged_weights: bfloat16 [8, 2560, 3072], P('expert', None, 'mp')
The draws below stay inside these ranges and needn't reach their ends.
Inputs may be any that keep to these rules, and one draw needn't show every extreme that they name: A permutation: expert e is held in serving position owner_map[e], by the serving group owner_map[e] // 2. `block_ids`: every slot of device s for owner q, used or not, names a block (e * 20 + r) * 24 + c with owner_map[e] // 2 == q // 2 and c // 12 == q % 2. Names may repeat within and across devices. `block_counts`: at most 2 used slots from one device to one owner; in every draw some owner receives exactly 2 blocks from every device.
All inputs are finite; a program needn't handle non-finite values.
Results may differ from the reference program's by a relative error of at most 0.001.
Values may be sent and summed in bfloat16 or wider, within the bound.
No kernel may reach another device: no remote copies, remote signals or barrier semaphores. Data moves between devices by JAX's collectives and lax.ppermute only.
A program may use at most 192 MiB of HBM per device.

```python
import jax
import jax.numpy as jnp
from jax import lax

BS = 128
DW = 2560
FF2 = 3072
EXP_DEV = 2
CAP = 2
E = 8
N_DEST = 8
RBW = 20
CB = 24
CBD = 12
N_MP = 2
DEVICES = 32


def serving_order(key):
    return jax.random.permutation(jax.random.fold_in(key, 11), E).astype(jnp.int32)


def draw_owner_map(key, part):
    return serving_order(key)


def draw_block_ids(key, part):
    order = serving_order(key)
    inverse = jnp.zeros((E,), jnp.int32).at[order].set(jnp.arange(E, dtype=jnp.int32))
    length = DEVICES * N_DEST * CAP
    slots = jnp.arange(length, dtype=jnp.int32)
    group = slots // CAP % N_DEST
    owner = group // N_MP
    column_part = group % N_MP
    within = jax.random.randint(jax.random.fold_in(key, 31), (length,), 0, EXP_DEV).astype(jnp.int32)
    expert = inverse[owner * EXP_DEV + within]
    row_pick = jax.random.randint(jax.random.fold_in(key, 32), (length,), 0, RBW).astype(jnp.int32)
    col_pick = jax.random.randint(jax.random.fold_in(key, 33), (length,), 0, CBD).astype(jnp.int32)
    column = column_part * CBD + col_pick
    return ((expert * RBW + row_pick) * CB + column).astype(jnp.int32)


def draw_block_counts(key, part):
    tiers = jax.random.randint(jax.random.fold_in(key, 21), (N_DEST,), 0, 4).astype(jnp.int32)
    fullest = jax.random.randint(jax.random.fold_in(key, 22), (), 0, N_DEST).astype(jnp.int32)
    tiers = jnp.where(jnp.arange(N_DEST, dtype=jnp.int32) == fullest, 0, tiers)
    limit = jnp.right_shift(jnp.int32(8), tiers)
    trials = jax.random.randint(jax.random.fold_in(key, 23), (DEVICES, N_DEST, CAP), 0, 8).astype(jnp.int32)
    counts = jnp.sum((trials < limit[None, :, None]).astype(jnp.int32), axis=2)
    return counts.reshape(DEVICES * N_DEST).astype(jnp.int32)


def steps_of(rng, shape, pieces, smallest, high):
    loudness, own = 1.0, jax.random.fold_in(rng, 6)
    for position, parts in pieces:
        heights = jnp.exp(jax.random.uniform(jax.random.fold_in(own, position), (parts,), jnp.float32, smallest / len(pieces), high / len(pieces)))
        loudness = loudness * jnp.repeat(heights, shape[position] // parts).reshape([-1 if axis == position else 1 for axis in range(len(shape))])
    return loudness


def gaussian(own_key, shape, width, bound, pieces=(), kind=jnp.bfloat16):
    entries = jax.random.normal(own_key, shape, jnp.float32) * width
    if len(pieces) > 0:
        entries = steps_of(own_key, shape, pieces, -0.22, 0.18) * entries
    return jnp.clip(entries, min=-bound, max=bound).astype(kind)


def setup_inputs(seed: int = 0) -> dict:
    key_of = jax.random.split(jax.random.key(seed), 6)
    return {
        "base_weights": gaussian(key_of[0], (E, DW, FF2), 1.0, 6.0, ((0, 4), (2, 2))),
        "delta_blocks": gaussian(key_of[1], (DEVICES * N_DEST * CAP, BS, BS), 0.5, 4.0, ((0, 32),)),
        "block_ids": draw_block_ids(jax.random.fold_in(key_of[5], 71), 0),
        "block_counts": draw_block_counts(jax.random.fold_in(key_of[5], 71), 0),
        "owner_map": draw_owner_map(jax.random.fold_in(key_of[5], 71), 0),
    }


def reference(base_weights, delta_blocks, block_ids, block_counts, owner_map):
    slot_count = N_DEST * CAP
    row_blocks = DW // BS
    col_total = FF2 // BS
    block_total = E * row_blocks * col_total
    listed = delta_blocks.reshape(DEVICES, slot_count, BS, BS)
    idents = block_ids.reshape(DEVICES, slot_count)
    counts = block_counts.reshape(DEVICES, N_DEST)
    active = (jnp.arange(slot_count, dtype=jnp.int32) % CAP)[None, :] < jnp.repeat(counts, CAP, axis=1)

    def add_source(running, record):
        values, names, usable = record
        values = jnp.where(usable[:, None, None], values.astype(jnp.float32), jnp.float32(0.0))
        return running.at[names].add(values), None

    start = jnp.zeros((block_total, BS, BS), jnp.float32)
    summed, unused = lax.scan(add_source, start, (listed, idents, active))
    grid = summed.reshape(E, row_blocks, col_total, BS, BS).transpose(0, 1, 3, 2, 4)
    task_delta = grid.reshape(E, DW, FF2)
    serving = jnp.zeros((E, DW, FF2), jnp.float32).at[owner_map].set(task_delta)
    return (base_weights.astype(jnp.float32) + serving).astype(jnp.bfloat16)
```

```python
import functools

import jax
import jax.numpy as jnp
from jax import lax
from jax.experimental import pallas as pl
from jax.experimental.pallas import tpu as pltpu
from jax.sharding import PartitionSpec as P


def source(index, step, size):
    if size & (size - 1) == 0:
        return index ^ step
    return (index - step) % size


def target(index, step, size):
    if size & (size - 1) == 0:
        return index ^ step
    return (index + step) % size


def add_blocks(ids_ref, *refs, pieces, slots, row_blocks, col_blocks, block, exp_dev):
    arrived = refs[:pieces]
    out = refs[pieces + 1]
    delta, total, held, counts, places, in_sem, read_sem, write_sem = refs[pieces + 2:]
    per_piece = arrived[0].shape[0]
    by_slot = slots <= exp_dev * row_blocks * col_blocks

    def piece_copy(j):
        return pltpu.make_async_copy(
            arrived[j], delta.at[pl.ds(j * per_piece, per_piece)], in_sem.at[j]
        )

    for j in range(pieces):
        piece_copy(j).start()

    def place_of(ident):
        expert = ident // (row_blocks * col_blocks)
        remain = ident % (row_blocks * col_blocks)
        row = pl.multiple_of(remain // col_blocks * block, block)
        col = pl.multiple_of(remain % col_blocks * block, block)
        return out.at[expert, pl.ds(row, block), pl.ds(col, block)]

    def read(ident, k):
        return pltpu.make_async_copy(place_of(ident), held.at[k], read_sem.at[k])

    def write(ident, k):
        return pltpu.make_async_copy(held.at[k], place_of(ident), write_sem.at[k])

    def clear(i, carry):
        counts[jnp.maximum(ids_ref[i], 0)] = 0
        return carry

    lax.fori_loop(0, slots, clear, 0)

    def count(i, carry):
        ident = ids_ref[i]

        @pl.when(ident >= 0)
        def _():
            seen = counts[ident]
            counts[ident] = seen + 1

            @pl.when(seen == 0)
            def _():
                k = i if by_slot else ident
                places[ident] = k
                read(ident, k).start()

        return carry

    lax.fori_loop(0, slots, count, 0)

    def combine(i, carry):
        ident = ids_ref[i]

        @pl.when(ident >= 0)
        def _():
            k = places[ident]
            left = counts[ident]
            first = (i == k) if by_slot else (left > 0)
            single = jnp.logical_and(first, left == 1)
            remaining = jnp.where(left > 0, left, -left) - 1
            counts[ident] = -remaining
            here = delta[i].astype(jnp.float32)

            @pl.when(single)
            def _():
                read(ident, k).wait()
                held[k] = (held[k].astype(jnp.float32) + here).astype(jnp.bfloat16)
                write(ident, k).start()

            @pl.when(jnp.logical_not(single))
            def _():
                @pl.when(first)
                def _():
                    total[k] = here

                @pl.when(jnp.logical_not(first))
                def _():
                    total[k] = total[k] + here

                @pl.when(remaining == 0)
                def _():
                    read(ident, k).wait()
                    held[k] = (held[k].astype(jnp.float32) + total[k]).astype(jnp.bfloat16)
                    write(ident, k).start()

        return carry

    for j in range(pieces):
        piece_copy(j).wait()
        lax.fori_loop(j * per_piece, (j + 1) * per_piece, combine, 0)

    def finish(i, carry):
        ident = ids_ref[i]

        @pl.when(ident >= 0)
        def _():
            @pl.when(counts[ident] == 0)
            def _():
                counts[ident] = 1
                write(ident, places[ident]).wait()

        return carry

    lax.fori_loop(0, slots, finish, 0)


def body(base_weights, delta_blocks, block_ids, block_counts, owner_map):
    exp_dev, row_count, col_count = base_weights.shape
    block = delta_blocks.shape[1]
    row_blocks = row_count // block
    col_blocks = col_count // block
    mp_size = lax.axis_size("mp")
    dp_size = lax.axis_size("dp")
    group_size = lax.axis_size("expert") * mp_size
    col_total = col_blocks * mp_size
    slot_total = delta_blocks.shape[0]
    capacity = slot_total // group_size
    rank = lax.axis_index("expert") * mp_size + lax.axis_index("mp")
    copy_index = lax.axis_index("dp")

    parts = []
    for step in range(group_size):
        sent = lax.dynamic_slice_in_dim(
            delta_blocks, target(rank, step, group_size) * capacity, capacity, 0
        )
        if step:
            pairs = [(i, target(i, step, group_size)) for i in range(group_size)]
            sent = lax.ppermute(sent, ("expert", "mp"), pairs)
        parts.append(sent)
    own = jnp.concatenate(parts, axis=0)
    pieces = [own]
    for step in range(1, dp_size):
        pairs = [(i, target(i, step, dp_size)) for i in range(dp_size)]
        pieces.append(lax.ppermute(own, "dp", pairs))

    active = (
        jnp.arange(capacity, dtype=jnp.int32)[None, :] < block_counts[:, None]
    )
    expert = block_ids // (row_blocks * col_total)
    remain = block_ids % (row_blocks * col_total)
    expert_count = owner_map.shape[0]
    matches = expert[:, None] == jnp.arange(expert_count, dtype=jnp.int32)[None, :]
    position = jnp.sum(jnp.where(matches, owner_map[None, :], 0), axis=1)
    idents = (
        position % exp_dev * row_blocks + remain // col_total
    ) * col_blocks + remain % col_total % col_blocks
    idents = jnp.where(active, idents.reshape(group_size, capacity), -1)
    every = lax.all_gather(idents, ("dp", "expert", "mp"), axis=0, tiled=True)
    every = every.reshape(dp_size, group_size, group_size, capacity)
    mine = lax.dynamic_slice_in_dim(every, rank, 1, 2).reshape(dp_size, group_size, capacity)
    rows = []
    for s in range(dp_size):
        from_copy = source(copy_index, s, dp_size)
        owner_rows = lax.dynamic_slice_in_dim(mine, from_copy, 1, 0)[0]
        rows.append(owner_rows)
    ordered = jnp.stack(rows)
    group_order = jnp.stack([source(rank, s, group_size) for s in range(group_size)])
    pick = group_order[:, None] == jnp.arange(group_size, dtype=jnp.int32)[None, :]
    ordered = jnp.sum(
        jnp.where(pick[None, :, :, None], ordered[:, None, :, :], 0), axis=2
    ).reshape(-1)

    slots = dp_size * slot_total
    block_total = exp_dev * row_blocks * col_blocks
    kept = min(slots, block_total)
    return pl.pallas_call(
        functools.partial(
            add_blocks, pieces=dp_size, slots=slots, row_blocks=row_blocks,
            col_blocks=col_blocks, block=block, exp_dev=exp_dev,
        ),
        out_shape=jax.ShapeDtypeStruct(base_weights.shape, base_weights.dtype),
        in_specs=[pl.BlockSpec(memory_space=pltpu.SMEM)]
        + [pl.BlockSpec(memory_space=pl.ANY)] * (dp_size + 1),
        out_specs=pl.BlockSpec(memory_space=pl.ANY),
        scratch_shapes=[
            pltpu.VMEM((slots, block, block), jnp.bfloat16),
            pltpu.VMEM((kept, block, block), jnp.float32),
            pltpu.VMEM((kept, block, block), jnp.bfloat16),
            pltpu.SMEM((block_total,), jnp.int32),
            pltpu.SMEM((block_total,), jnp.int32),
            pltpu.SemaphoreType.DMA((dp_size,)),
            pltpu.SemaphoreType.DMA((kept,)),
            pltpu.SemaphoreType.DMA((kept,)),
        ],
        input_output_aliases={dp_size + 1: 0},
    )(ordered, *pieces, base_weights)


def solution(mesh):
    in_specs = (
        P("expert", None, "mp"),
        P(("dp", "expert", "mp"), None, None),
        P(("dp", "expert", "mp")),
        P(("dp", "expert", "mp")),
        P(),
    )
    out_specs = P("expert", None, "mp")
    return jax.shard_map(body, mesh=mesh, in_specs=in_specs, out_specs=out_specs, check_vma=False)
```

```python
import functools

import jax
import jax.numpy as jnp
from jax import lax
from jax.experimental import pallas as pl
from jax.experimental.pallas import tpu as pltpu
from jax.sharding import PartitionSpec as P


def source(index, step, size):
    if size & (size - 1) == 0:
        return index ^ step
    return (index - step) % size


def target(index, step, size):
    if size & (size - 1) == 0:
        return index ^ step
    return (index + step) % size


def add_blocks(ids_ref, *refs, pieces, slots, row_blocks, col_blocks, block, exp_dev):
    arrived = refs[:pieces]
    out = refs[pieces + 1]
    delta, total, held, counts, places, in_sem, read_sem, write_sem = refs[pieces + 2:]
    per_piece = arrived[0].shape[0]
    by_slot = slots <= exp_dev * row_blocks * col_blocks

    def piece_copy(j):
        return pltpu.make_async_copy(
            arrived[j], delta.at[pl.ds(j * per_piece, per_piece)], in_sem.at[j]
        )

    for j in range(pieces):
        piece_copy(j).start()

    def place_of(ident):
        expert = ident // (row_blocks * col_blocks)
        remain = ident % (row_blocks * col_blocks)
        row = pl.multiple_of(remain // col_blocks * block, block)
        col = pl.multiple_of(remain % col_blocks * block, block)
        return out.at[expert, pl.ds(row, block), pl.ds(col, block)]

    def read(ident, k):
        return pltpu.make_async_copy(place_of(ident), held.at[k], read_sem.at[k])

    def write(ident, k):
        return pltpu.make_async_copy(held.at[k], place_of(ident), write_sem.at[k])

    def clear(i, carry):
        counts[jnp.maximum(ids_ref[i], 0)] = 0
        return carry

    lax.fori_loop(0, slots, clear, 0)

    def count(i, carry):
        ident = ids_ref[i]

        @pl.when(ident >= 0)
        def _():
            seen = counts[ident]
            counts[ident] = seen + 1

            @pl.when(seen == 0)
            def _():
                k = i if by_slot else ident
                places[ident] = k
                read(ident, k).start()

        return carry

    lax.fori_loop(0, slots, count, 0)

    def combine(i, carry):
        ident = ids_ref[i]

        @pl.when(ident >= 0)
        def _():
            k = places[ident]
            left = counts[ident]
            first = (i == k) if by_slot else (left > 0)
            single = jnp.logical_and(first, left == 1)
            remaining = jnp.where(left > 0, left, -left) - 1
            counts[ident] = -remaining
            here = delta[i].astype(jnp.float32)

            @pl.when(single)
            def _():
                read(ident, k).wait()
                held[k] = (held[k].astype(jnp.float32) + here).astype(jnp.bfloat16)
                write(ident, k).start()

            @pl.when(jnp.logical_not(single))
            def _():
                @pl.when(first)
                def _():
                    total[k] = here

                @pl.when(jnp.logical_not(first))
                def _():
                    total[k] = total[k] + here

                @pl.when(remaining == 0)
                def _():
                    read(ident, k).wait()
                    held[k] = (held[k].astype(jnp.float32) + total[k]).astype(jnp.bfloat16)
                    write(ident, k).start()

        return carry

    for j in range(pieces):
        piece_copy(j).wait()
        lax.fori_loop(j * per_piece, (j + 1) * per_piece, combine, 0)

    def finish(i, carry):
        ident = ids_ref[i]

        @pl.when(ident >= 0)
        def _():
            @pl.when(counts[ident] == 0)
            def _():
                counts[ident] = 1
                write(ident, places[ident]).wait()

        return carry

    lax.fori_loop(0, slots, finish, 0)


def over_dp(array, step, size):
    return lax.ppermute(array, "dp", [(i, target(i, step, size)) for i in range(size)])


def copy_base(base_weights, after, rows):
    def copy(base_ref, after_ref, out_ref):
        out_ref[...] = base_ref[...]

    exp_dev, row_count, col_count = base_weights.shape
    spec = pl.BlockSpec((1, rows, col_count), lambda e, r: (e, r, 0))
    return pl.pallas_call(
        copy,
        out_shape=jax.ShapeDtypeStruct(base_weights.shape, base_weights.dtype),
        grid=(exp_dev, row_count // rows),
        in_specs=[spec, pl.BlockSpec(memory_space=pl.ANY)],
        out_specs=spec,
    )(base_weights, after)


def body(base_weights, delta_blocks, block_ids, block_counts, owner_map):
    exp_dev, row_count, col_count = base_weights.shape
    block = delta_blocks.shape[1]
    row_blocks = row_count // block
    col_blocks = col_count // block
    mp_size = lax.axis_size("mp")
    dp_size = lax.axis_size("dp")
    group_size = lax.axis_size("expert") * mp_size
    col_total = col_blocks * mp_size
    slot_total = delta_blocks.shape[0]
    capacity = slot_total // group_size
    rank = lax.axis_index("expert") * mp_size + lax.axis_index("mp")

    active = (
        jnp.arange(capacity, dtype=jnp.int32)[None, :] < block_counts[:, None]
    )
    expert = block_ids // (row_blocks * col_total)
    remain = block_ids % (row_blocks * col_total)
    expert_count = owner_map.shape[0]
    matches = expert[:, None] == jnp.arange(expert_count, dtype=jnp.int32)[None, :]
    position = jnp.sum(jnp.where(matches, owner_map[None, :], 0), axis=1)
    idents = (
        position % exp_dev * row_blocks + remain // col_total
    ) * col_blocks + remain % col_total % col_blocks
    idents = jnp.where(active, idents.reshape(group_size, capacity), -1)
    came = lax.all_to_all(idents, ("expert", "mp"), split_axis=0, concat_axis=0, tiled=True)
    group_order = jnp.stack([source(rank, s, group_size) for s in range(group_size)])
    pick = group_order[:, None] == jnp.arange(group_size, dtype=jnp.int32)[None, :]
    came = jnp.sum(jnp.where(pick[:, :, None], came[None, :, :], 0), axis=1).reshape(-1)
    came_all = [came] + [over_dp(came, step, dp_size) for step in range(1, dp_size)]

    parts = []
    for step in range(group_size):
        sent = lax.dynamic_slice_in_dim(
            delta_blocks, target(rank, step, group_size) * capacity, capacity, 0
        )
        if step:
            pairs = [(i, target(i, step, group_size)) for i in range(group_size)]
            sent = lax.ppermute(sent, ("expert", "mp"), pairs)
        parts.append(sent)
    half = group_size // 2
    near = jnp.concatenate(parts[:half], axis=0)
    far = jnp.concatenate(parts[half:], axis=0)
    if dp_size == 4:
        near_1, far_2 = over_dp(near, 1, 4), over_dp(far, 2, 4)
        near_2, far_1 = over_dp(near, 2, 4), over_dp(far, 1, 4)
        nears = [near, near_1, near_2, over_dp(near_1, 2, 4)]
        fars = [far, far_1, far_2, over_dp(far_2, 1, 4)]
    else:
        nears = [near] + [over_dp(near, step, dp_size) for step in range(1, dp_size)]
        fars = [far] + [over_dp(far, step, dp_size) for step in range(1, dp_size)]
    pieces = nears + fars
    cut = half * capacity
    ordered = jnp.concatenate([c[:cut] for c in came_all] + [c[cut:] for c in came_all])
    copied = copy_base(base_weights, far, block * 2 if row_blocks % 2 == 0 else block)

    slots = dp_size * slot_total
    block_total = exp_dev * row_blocks * col_blocks
    kept = min(slots, block_total)
    return pl.pallas_call(
        functools.partial(
            add_blocks, pieces=len(pieces), slots=slots, row_blocks=row_blocks,
            col_blocks=col_blocks, block=block, exp_dev=exp_dev,
        ),
        out_shape=jax.ShapeDtypeStruct(base_weights.shape, base_weights.dtype),
        in_specs=[pl.BlockSpec(memory_space=pltpu.SMEM)]
        + [pl.BlockSpec(memory_space=pl.ANY)] * (len(pieces) + 1),
        out_specs=pl.BlockSpec(memory_space=pl.ANY),
        scratch_shapes=[
            pltpu.VMEM((slots, block, block), jnp.bfloat16),
            pltpu.VMEM((kept, block, block), jnp.float32),
            pltpu.VMEM((kept, block, block), jnp.bfloat16),
            pltpu.SMEM((block_total,), jnp.int32),
            pltpu.SMEM((block_total,), jnp.int32),
            pltpu.SemaphoreType.DMA((len(pieces),)),
            pltpu.SemaphoreType.DMA((kept,)),
            pltpu.SemaphoreType.DMA((kept,)),
        ],
        input_output_aliases={len(pieces) + 1: 0},
    )(ordered, *pieces, copied)


def solution(mesh):
    in_specs = (
        P("expert", None, "mp"),
        P(("dp", "expert", "mp"), None, None),
        P(("dp", "expert", "mp")),
        P(("dp", "expert", "mp")),
        P(),
    )
    out_specs = P("expert", None, "mp")
    return jax.shard_map(body, mesh=mesh, in_specs=in_specs, out_specs=out_specs, check_vma=False)
```

```python
import functools

import jax
import jax.numpy as jnp
from jax import lax
from jax.experimental import pallas as pl
from jax.experimental.pallas import tpu as pltpu
from jax.sharding import PartitionSpec as P


def source(index, step, size):
    if size & (size - 1) == 0:
        return index ^ step
    return (index - step) % size


def target(index, step, size):
    if size & (size - 1) == 0:
        return index ^ step
    return (index + step) % size


def add_blocks(ids_ref, *refs, pieces, slots, row_blocks, col_blocks, block, exp_dev):
    arrived = refs[:pieces]
    out = refs[pieces + 1]
    total, held, counts, places, read_sem, write_sem = refs[pieces + 2:]
    per_piece = arrived[0].shape[0]
    by_slot = slots <= exp_dev * row_blocks * col_blocks

    def place_of(ident):
        expert = ident // (row_blocks * col_blocks)
        remain = ident % (row_blocks * col_blocks)
        row = pl.multiple_of(remain // col_blocks * block, block)
        col = pl.multiple_of(remain % col_blocks * block, block)
        return out.at[expert, pl.ds(row, block), pl.ds(col, block)]

    def read(ident, k):
        return pltpu.make_async_copy(place_of(ident), held.at[k], read_sem.at[k])

    def write(ident, k):
        return pltpu.make_async_copy(held.at[k], place_of(ident), write_sem.at[k])

    def clear(i, carry):
        counts[jnp.maximum(ids_ref[i], 0)] = 0
        return carry

    lax.fori_loop(0, slots, clear, 0)

    def count(i, carry):
        ident = ids_ref[i]

        @pl.when(ident >= 0)
        def _():
            seen = counts[ident]
            counts[ident] = seen + 1

            @pl.when(seen == 0)
            def _():
                k = i if by_slot else ident
                places[ident] = k
                read(ident, k).start()

        return carry

    lax.fori_loop(0, slots, count, 0)

    def combine(i, carry, j):
        ident = ids_ref[i]

        @pl.when(ident >= 0)
        def _():
            k = places[ident]
            left = counts[ident]
            first = (i == k) if by_slot else (left > 0)
            single = jnp.logical_and(first, left == 1)
            remaining = jnp.where(left > 0, left, -left) - 1
            counts[ident] = -remaining
            here = arrived[j][i - j * per_piece].astype(jnp.float32)

            @pl.when(single)
            def _():
                read(ident, k).wait()
                held[k] = (held[k].astype(jnp.float32) + here).astype(jnp.bfloat16)
                write(ident, k).start()

            @pl.when(jnp.logical_not(single))
            def _():
                @pl.when(first)
                def _():
                    total[k] = here

                @pl.when(jnp.logical_not(first))
                def _():
                    total[k] = total[k] + here

                @pl.when(remaining == 0)
                def _():
                    read(ident, k).wait()
                    held[k] = (held[k].astype(jnp.float32) + total[k]).astype(jnp.bfloat16)
                    write(ident, k).start()

        return carry

    for j in range(pieces):
        lax.fori_loop(
            j * per_piece, (j + 1) * per_piece, functools.partial(combine, j=j), 0
        )

    def finish(i, carry):
        ident = ids_ref[i]

        @pl.when(ident >= 0)
        def _():
            @pl.when(counts[ident] == 0)
            def _():
                counts[ident] = 1
                write(ident, places[ident]).wait()

        return carry

    lax.fori_loop(0, slots, finish, 0)


def shifted(array, axis, step, size):
    if step == 0:
        return array
    return lax.ppermute(array, axis, [(i, target(i, step, size)) for i in range(size)])


def over_dp(array, step, size):
    return shifted(array, "dp", step, size)


def copy_base(base_weights, afters, rows):
    def copy(base_ref, *refs):
        refs[-1][...] = base_ref[...]

    exp_dev, row_count, col_count = base_weights.shape
    flat = base_weights.reshape(exp_dev * row_count, col_count)
    chunks = exp_dev * row_count // rows
    out = None
    for part, after in enumerate(afters):
        low = chunks * part // len(afters)
        high = chunks * (part + 1) // len(afters)
        spec = pl.BlockSpec((rows, col_count), lambda r, low=low: (r + low, 0))
        held = [after] if out is None else [after, out]
        out = pl.pallas_call(
            copy,
            out_shape=jax.ShapeDtypeStruct(flat.shape, flat.dtype),
            grid=(high - low,),
            in_specs=[spec] + [pl.BlockSpec(memory_space=pl.ANY)] * len(held),
            out_specs=spec,
            input_output_aliases={} if out is None else {2: 0},
            cost_estimate=pl.CostEstimate(
                flops=0, transcendentals=0, bytes_accessed=(high - low) * rows * col_count * 4
            ),
        )(flat, *held)
    return out.reshape(base_weights.shape)


def body(base_weights, delta_blocks, block_ids, block_counts, owner_map):
    exp_dev, row_count, col_count = base_weights.shape
    block = delta_blocks.shape[1]
    row_blocks = row_count // block
    col_blocks = col_count // block
    mp_size = lax.axis_size("mp")
    dp_size = lax.axis_size("dp")
    group_size = lax.axis_size("expert") * mp_size
    col_total = col_blocks * mp_size
    slot_total = delta_blocks.shape[0]
    capacity = slot_total // group_size
    mp_index = lax.axis_index("mp")
    expert_index = lax.axis_index("expert")
    copy_index = lax.axis_index("dp")

    expert_size = group_size // mp_size
    laid = delta_blocks.reshape(expert_size, mp_size, capacity, block, block)
    stages = []
    for step in range(mp_size):
        sent = lax.dynamic_slice_in_dim(laid, target(mp_index, step, mp_size), 1, 1)
        stages.append(shifted(sent, "mp", step, mp_size))
    gathered = jnp.concatenate(stages, axis=1)
    parts = []
    for step in range(expert_size):
        sent = lax.dynamic_slice_in_dim(gathered, target(expert_index, step, expert_size), 1, 0)
        sent = sent.reshape(mp_size * capacity, block, block)
        parts.append(shifted(sent, "expert", step, expert_size))
    half = expert_size // 2
    near = jnp.concatenate(parts[:half], axis=0)
    far = jnp.concatenate(parts[half:], axis=0)

    active = (
        jnp.arange(capacity, dtype=jnp.int32)[None, :] < block_counts[:, None]
    )
    block_ids, unused = lax.optimization_barrier((block_ids, stages[-1]))
    expert = block_ids // (row_blocks * col_total)
    remain = block_ids % (row_blocks * col_total)
    expert_count = owner_map.shape[0]
    matches = expert[:, None] == jnp.arange(expert_count, dtype=jnp.int32)[None, :]
    position = jnp.sum(jnp.where(matches, owner_map[None, :], 0), axis=1)
    idents = (
        position % exp_dev * row_blocks + remain // col_total
    ) * col_blocks + remain % col_total % col_blocks
    idents = jnp.where(active, idents.reshape(group_size, capacity), -1)
    idents = jnp.tile(idents, (dp_size, 1))
    came = lax.all_to_all(
        idents, ("dp", "expert", "mp"), split_axis=0, concat_axis=0, tiled=True
    )
    lie = [
        (source(copy_index, d, dp_size) * expert_size + source(expert_index, s, expert_size)) * mp_size
        + source(mp_index, t, mp_size)
        for part in (range(half), range(half, expert_size))
        for d in range(dp_size)
        for s in part
        for t in range(mp_size)
    ]
    device_count = dp_size * group_size
    pick = jnp.stack(lie)[:, None] == jnp.arange(device_count, dtype=jnp.int32)[None, :]
    ordered = jnp.sum(jnp.where(pick[:, :, None], came[None, :, :], 0), axis=1).reshape(-1)

    if dp_size == 4:
        near_1, far_2 = over_dp(near, 1, 4), over_dp(far, 2, 4)
        near_2, far_1 = over_dp(near, 2, 4), over_dp(far, 1, 4)
        nears = [near, near_1, near_2, over_dp(near_1, 2, 4)]
        fars = [far, far_1, far_2, over_dp(far_2, 1, 4)]
    else:
        nears = [near] + [over_dp(near, step, dp_size) for step in range(1, dp_size)]
        fars = [far] + [over_dp(far, step, dp_size) for step in range(1, dp_size)]
    pieces = nears + fars
    copied = copy_base(base_weights, (parts[0], far, nears[1]), block * 4)

    slots = dp_size * slot_total
    block_total = exp_dev * row_blocks * col_blocks
    kept = min(slots, block_total)
    return pl.pallas_call(
        functools.partial(
            add_blocks, pieces=len(pieces), slots=slots, row_blocks=row_blocks,
            col_blocks=col_blocks, block=block, exp_dev=exp_dev,
        ),
        out_shape=jax.ShapeDtypeStruct(base_weights.shape, base_weights.dtype),
        in_specs=[pl.BlockSpec(memory_space=pltpu.SMEM)]
        + [pl.BlockSpec(memory_space=pltpu.VMEM)] * len(pieces)
        + [pl.BlockSpec(memory_space=pl.ANY)],
        out_specs=pl.BlockSpec(memory_space=pl.ANY),
        scratch_shapes=[
            pltpu.VMEM((kept, block, block), jnp.float32),
            pltpu.VMEM((kept, block, block), jnp.bfloat16),
            pltpu.SMEM((block_total,), jnp.int32),
            pltpu.SMEM((block_total,), jnp.int32),
            pltpu.SemaphoreType.DMA((kept,)),
            pltpu.SemaphoreType.DMA((kept,)),
        ],
        input_output_aliases={len(pieces) + 1: 0},
    )(ordered, *pieces, copied)


def solution(mesh):
    in_specs = (
        P("expert", None, "mp"),
        P(("dp", "expert", "mp"), None, None),
        P(("dp", "expert", "mp")),
        P(("dp", "expert", "mp")),
        P(),
    )
    out_specs = P("expert", None, "mp")
    return jax.shard_map(body, mesh=mesh, in_specs=in_specs, out_specs=out_specs, check_vma=False)
```

```python
import functools

import jax
import jax.numpy as jnp
from jax import lax
from jax.experimental import pallas as pl
from jax.experimental.pallas import tpu as pltpu
from jax.sharding import PartitionSpec as P


def source(index, step, size):
    if size & (size - 1) == 0:
        return index ^ step
    return (index - step) % size


def target(index, step, size):
    if size & (size - 1) == 0:
        return index ^ step
    return (index + step) % size


def add_blocks(ids_ref, *refs, pieces, slots, row_blocks, col_blocks, block, exp_dev):
    arrived = refs[:pieces]
    out = refs[pieces + 1]
    total, held, counts, places, read_sem, write_sem = refs[pieces + 2:]
    per_piece = arrived[0].shape[0]
    by_slot = slots <= exp_dev * row_blocks * col_blocks

    def place_of(ident):
        expert = ident // (row_blocks * col_blocks)
        remain = ident % (row_blocks * col_blocks)
        row = pl.multiple_of(remain // col_blocks * block, block)
        col = pl.multiple_of(remain % col_blocks * block, block)
        return out.at[expert, pl.ds(row, block), pl.ds(col, block)]

    def read(ident, k):
        return pltpu.make_async_copy(place_of(ident), held.at[k], read_sem.at[k])

    def write(ident, k):
        return pltpu.make_async_copy(held.at[k], place_of(ident), write_sem.at[k])

    def clear(i, carry):
        counts[jnp.maximum(ids_ref[i], 0)] = 0
        return carry

    lax.fori_loop(0, slots, clear, 0)

    def count(i, carry):
        ident = ids_ref[i]

        @pl.when(ident >= 0)
        def _():
            seen = counts[ident]
            counts[ident] = seen + 1

            @pl.when(seen == 0)
            def _():
                k = i if by_slot else ident
                places[ident] = k
                read(ident, k).start()

        return carry

    lax.fori_loop(0, slots, count, 0)

    def combine(i, carry, j):
        ident = ids_ref[i]

        @pl.when(ident >= 0)
        def _():
            k = places[ident]
            left = counts[ident]
            first = (i == k) if by_slot else (left > 0)
            single = jnp.logical_and(first, left == 1)
            remaining = jnp.where(left > 0, left, -left) - 1
            counts[ident] = -remaining
            here = arrived[j][i - j * per_piece].astype(jnp.float32)

            @pl.when(single)
            def _():
                read(ident, k).wait()
                held[k] = (held[k].astype(jnp.float32) + here).astype(jnp.bfloat16)
                write(ident, k).start()

            @pl.when(jnp.logical_not(single))
            def _():
                @pl.when(first)
                def _():
                    total[k] = here

                @pl.when(jnp.logical_not(first))
                def _():
                    total[k] = total[k] + here

                @pl.when(remaining == 0)
                def _():
                    read(ident, k).wait()
                    held[k] = (held[k].astype(jnp.float32) + total[k]).astype(jnp.bfloat16)
                    write(ident, k).start()

        return carry

    for j in range(pieces):
        lax.fori_loop(
            j * per_piece, (j + 1) * per_piece, functools.partial(combine, j=j), 0
        )

    def finish(i, carry):
        ident = ids_ref[i]

        @pl.when(ident >= 0)
        def _():
            @pl.when(counts[ident] == 0)
            def _():
                counts[ident] = 1
                write(ident, places[ident]).wait()

        return carry

    lax.fori_loop(0, slots, finish, 0)


def shifted(array, axis, step, size):
    if step == 0:
        return array
    return lax.ppermute(array, axis, [(i, target(i, step, size)) for i in range(size)])


def over_dp(array, step, size):
    return shifted(array, "dp", step, size)


def copy_base(base_weights, afters, rows):
    def copy(base_ref, *refs):
        refs[-1][...] = base_ref[...]

    exp_dev, row_count, col_count = base_weights.shape
    flat = base_weights.reshape(exp_dev * row_count, col_count)
    chunks = exp_dev * row_count // rows
    out = None
    for part, after in enumerate(afters):
        low = chunks * part // len(afters)
        high = chunks * (part + 1) // len(afters)
        spec = pl.BlockSpec((rows, col_count), lambda r, low=low: (r + low, 0))
        held = [after] if out is None else [after, out]
        out = pl.pallas_call(
            copy,
            out_shape=jax.ShapeDtypeStruct(flat.shape, flat.dtype),
            grid=(high - low,),
            in_specs=[spec] + [pl.BlockSpec(memory_space=pl.ANY)] * len(held),
            out_specs=spec,
            input_output_aliases={} if out is None else {2: 0},
            cost_estimate=pl.CostEstimate(
                flops=0, transcendentals=0, bytes_accessed=(high - low) * rows * col_count * 4
            ),
        )(flat, *held)
    return out.reshape(base_weights.shape)


def body(base_weights, delta_blocks, block_ids, block_counts, owner_map):
    exp_dev, row_count, col_count = base_weights.shape
    block = delta_blocks.shape[1]
    row_blocks = row_count // block
    col_blocks = col_count // block
    mp_size = lax.axis_size("mp")
    dp_size = lax.axis_size("dp")
    group_size = lax.axis_size("expert") * mp_size
    col_total = col_blocks * mp_size
    slot_total = delta_blocks.shape[0]
    capacity = slot_total // group_size
    mp_index = lax.axis_index("mp")
    expert_index = lax.axis_index("expert")
    copy_index = lax.axis_index("dp")

    expert_size = group_size // mp_size
    laid = delta_blocks.reshape(expert_size, mp_size, capacity, block, block)
    stages = []
    for step in range(mp_size):
        sent = lax.dynamic_slice_in_dim(laid, target(mp_index, step, mp_size), 1, 1)
        stages.append(shifted(sent, "mp", step, mp_size))
    gathered = jnp.concatenate(stages, axis=1)
    parts = []
    for step in range(expert_size):
        sent = lax.dynamic_slice_in_dim(gathered, target(expert_index, step, expert_size), 1, 0)
        sent = sent.reshape(mp_size * capacity, block, block)
        parts.append(shifted(sent, "expert", step, expert_size))
    half = expert_size // 2
    near = jnp.concatenate(parts[:half], axis=0)
    far = jnp.concatenate(parts[half:], axis=0)

    active = (
        jnp.arange(capacity, dtype=jnp.int32)[None, :] < block_counts[:, None]
    )
    block_ids, unused = lax.optimization_barrier((block_ids, stages[-1]))
    expert = block_ids // (row_blocks * col_total)
    remain = block_ids % (row_blocks * col_total)
    expert_count = owner_map.shape[0]
    matches = expert[:, None] == jnp.arange(expert_count, dtype=jnp.int32)[None, :]
    position = jnp.sum(jnp.where(matches, owner_map[None, :], 0), axis=1)
    idents = (
        position % exp_dev * row_blocks + remain // col_total
    ) * col_blocks + remain % col_total % col_blocks
    idents = jnp.where(active, idents.reshape(group_size, capacity), -1)
    idents = jnp.tile(idents, (dp_size, 1))
    came = lax.all_to_all(
        idents, ("dp", "expert", "mp"), split_axis=0, concat_axis=0, tiled=True
    )
    near, far, came = lax.optimization_barrier((near, far, came))
    lie = [
        (source(copy_index, d, dp_size) * expert_size + source(expert_index, s, expert_size)) * mp_size
        + source(mp_index, t, mp_size)
        for part in (range(half), range(half, expert_size))
        for d in range(dp_size)
        for s in part
        for t in range(mp_size)
    ]
    device_count = dp_size * group_size
    pick = jnp.stack(lie)[:, None] == jnp.arange(device_count, dtype=jnp.int32)[None, :]
    ordered = jnp.sum(jnp.where(pick[:, :, None], came[None, :, :], 0), axis=1).reshape(-1)

    if dp_size == 4:
        near_1, far_2 = over_dp(near, 1, 4), over_dp(far, 2, 4)
        near_2, far_1 = over_dp(near, 2, 4), over_dp(far, 1, 4)
        nears = [near, near_1, near_2, over_dp(near_1, 2, 4)]
        fars = [far, far_1, far_2, over_dp(far_2, 1, 4)]
    else:
        nears = [near] + [over_dp(near, step, dp_size) for step in range(1, dp_size)]
        fars = [far] + [over_dp(far, step, dp_size) for step in range(1, dp_size)]
    pieces = nears + fars
    copied = copy_base(base_weights, (parts[0], far, nears[1]), block * 4)

    slots = dp_size * slot_total
    block_total = exp_dev * row_blocks * col_blocks
    kept = min(slots, block_total)
    return pl.pallas_call(
        functools.partial(
            add_blocks, pieces=len(pieces), slots=slots, row_blocks=row_blocks,
            col_blocks=col_blocks, block=block, exp_dev=exp_dev,
        ),
        out_shape=jax.ShapeDtypeStruct(base_weights.shape, base_weights.dtype),
        in_specs=[pl.BlockSpec(memory_space=pltpu.SMEM)]
        + [pl.BlockSpec(memory_space=pltpu.VMEM)] * len(pieces)
        + [pl.BlockSpec(memory_space=pl.ANY)],
        out_specs=pl.BlockSpec(memory_space=pl.ANY),
        scratch_shapes=[
            pltpu.VMEM((kept, block, block), jnp.float32),
            pltpu.VMEM((kept, block, block), jnp.bfloat16),
            pltpu.SMEM((block_total,), jnp.int32),
            pltpu.SMEM((block_total,), jnp.int32),
            pltpu.SemaphoreType.DMA((kept,)),
            pltpu.SemaphoreType.DMA((kept,)),
        ],
        input_output_aliases={len(pieces) + 1: 0},
    )(ordered, *pieces, copied)


def solution(mesh):
    in_specs = (
        P("expert", None, "mp"),
        P(("dp", "expert", "mp"), None, None),
        P(("dp", "expert", "mp")),
        P(("dp", "expert", "mp")),
        P(),
    )
    out_specs = P("expert", None, "mp")
    return jax.shard_map(body, mesh=mesh, in_specs=in_specs, out_specs=out_specs, check_vma=False)
```

```python
import functools

import jax
import jax.numpy as jnp
from jax import lax
from jax.experimental import pallas as pl
from jax.experimental.pallas import tpu as pltpu
from jax.sharding import PartitionSpec as P


def source(index, step, size):
    if size & (size - 1) == 0:
        return index ^ step
    return (index - step) % size


def target(index, step, size):
    if size & (size - 1) == 0:
        return index ^ step
    return (index + step) % size


def add_blocks(ids_ref, *refs, pieces, slots, row_blocks, col_blocks, block, exp_dev):
    arrived = refs[:pieces]
    out = refs[pieces + 1]
    total, held, counts, places, read_sem, write_sem = refs[pieces + 2:]
    per_piece = arrived[0].shape[0]
    by_slot = slots <= exp_dev * row_blocks * col_blocks

    def place_of(ident):
        expert = ident // (row_blocks * col_blocks)
        remain = ident % (row_blocks * col_blocks)
        row = pl.multiple_of(remain // col_blocks * block, block)
        col = pl.multiple_of(remain % col_blocks * block, block)
        return out.at[expert, pl.ds(row, block), pl.ds(col, block)]

    def read(ident, k):
        return pltpu.make_async_copy(place_of(ident), held.at[k], read_sem.at[k])

    def write(ident, k):
        return pltpu.make_async_copy(held.at[k], place_of(ident), write_sem.at[k])

    def clear(i, carry):
        counts[jnp.maximum(ids_ref[i], 0)] = 0
        return carry

    lax.fori_loop(0, slots, clear, 0)

    def count(i, carry):
        ident = ids_ref[i]

        @pl.when(ident >= 0)
        def _():
            seen = counts[ident]
            counts[ident] = seen + 1

            @pl.when(seen == 0)
            def _():
                k = i if by_slot else ident
                places[ident] = k
                read(ident, k).start()

        return carry

    lax.fori_loop(0, slots, count, 0)

    def combine(i, carry, j):
        ident = ids_ref[i]

        @pl.when(ident >= 0)
        def _():
            k = places[ident]
            left = counts[ident]
            first = (i == k) if by_slot else (left > 0)
            single = jnp.logical_and(first, left == 1)
            remaining = jnp.where(left > 0, left, -left) - 1
            counts[ident] = -remaining
            here = arrived[j][i - j * per_piece].astype(jnp.float32)

            @pl.when(single)
            def _():
                read(ident, k).wait()
                held[k] = (held[k].astype(jnp.float32) + here).astype(jnp.bfloat16)
                write(ident, k).start()

            @pl.when(jnp.logical_not(single))
            def _():
                @pl.when(first)
                def _():
                    total[k] = here

                @pl.when(jnp.logical_not(first))
                def _():
                    total[k] = total[k] + here

                @pl.when(remaining == 0)
                def _():
                    read(ident, k).wait()
                    held[k] = (held[k].astype(jnp.float32) + total[k]).astype(jnp.bfloat16)
                    write(ident, k).start()

        return carry

    for j in range(pieces):
        lax.fori_loop(
            j * per_piece, (j + 1) * per_piece, functools.partial(combine, j=j), 0
        )

    def finish(i, carry):
        ident = ids_ref[i]

        @pl.when(ident >= 0)
        def _():
            @pl.when(counts[ident] == 0)
            def _():
                counts[ident] = 1
                write(ident, places[ident]).wait()

        return carry

    lax.fori_loop(0, slots, finish, 0)


def shifted(array, axis, step, size):
    if step == 0:
        return array
    return lax.ppermute(array, axis, [(i, target(i, step, size)) for i in range(size)])


def over_dp(array, step, size):
    return shifted(array, "dp", step, size)


def copy_base(base_weights, afters, rows, out=None, start=0, total=1):
    def copy(base_ref, *refs):
        refs[-1][...] = base_ref[...]

    exp_dev, row_count, col_count = base_weights.shape
    flat = base_weights.reshape(exp_dev * row_count, col_count)
    chunks = exp_dev * row_count // rows
    for part, after in enumerate(afters, start):
        low = chunks * part // total
        high = chunks * (part + 1) // total
        spec = pl.BlockSpec((rows, col_count), lambda r, low=low: (r + low, 0))
        held = [after] if out is None else [after, out]
        out = pl.pallas_call(
            copy,
            out_shape=jax.ShapeDtypeStruct(flat.shape, flat.dtype),
            grid=(high - low,),
            in_specs=[spec] + [pl.BlockSpec(memory_space=pl.ANY)] * len(held),
            out_specs=spec,
            input_output_aliases={} if out is None else {2: 0},
            cost_estimate=pl.CostEstimate(
                flops=0, transcendentals=0, bytes_accessed=(high - low) * rows * col_count * 4
            ),
        )(flat, *held)
    return out


def body(base_weights, delta_blocks, block_ids, block_counts, owner_map):
    exp_dev, row_count, col_count = base_weights.shape
    block = delta_blocks.shape[1]
    row_blocks = row_count // block
    col_blocks = col_count // block
    mp_size = lax.axis_size("mp")
    dp_size = lax.axis_size("dp")
    group_size = lax.axis_size("expert") * mp_size
    col_total = col_blocks * mp_size
    slot_total = delta_blocks.shape[0]
    capacity = slot_total // group_size
    mp_index = lax.axis_index("mp")
    expert_index = lax.axis_index("expert")
    copy_index = lax.axis_index("dp")

    expert_size = group_size // mp_size
    laid = delta_blocks.reshape(expert_size, mp_size, capacity, block, block)
    stages = []
    for step in range(mp_size):
        sent = lax.dynamic_slice_in_dim(laid, target(mp_index, step, mp_size), 1, 1)
        stages.append(shifted(sent, "mp", step, mp_size))
    gathered = jnp.concatenate(stages, axis=1)
    parts = []
    for step in range(expert_size):
        sent = lax.dynamic_slice_in_dim(gathered, target(expert_index, step, expert_size), 1, 0)
        sent = sent.reshape(mp_size * capacity, block, block)
        parts.append(shifted(sent, "expert", step, expert_size))
    half = expert_size // 2
    near = jnp.concatenate(parts[:half], axis=0)
    far = jnp.concatenate(parts[half:], axis=0)

    copied = copy_base(base_weights, (parts[0],), block * 4, total=3)
    near, far, copied = lax.optimization_barrier((near, far, copied))

    active = (
        jnp.arange(capacity, dtype=jnp.int32)[None, :] < block_counts[:, None]
    )
    block_ids, unused = lax.optimization_barrier((block_ids, stages[-1]))
    expert = block_ids // (row_blocks * col_total)
    remain = block_ids % (row_blocks * col_total)
    expert_count = owner_map.shape[0]
    matches = expert[:, None] == jnp.arange(expert_count, dtype=jnp.int32)[None, :]
    position = jnp.sum(jnp.where(matches, owner_map[None, :], 0), axis=1)
    idents = (
        position % exp_dev * row_blocks + remain // col_total
    ) * col_blocks + remain % col_total % col_blocks
    idents = jnp.where(active, idents.reshape(group_size, capacity), -1)
    idents = jnp.tile(idents, (dp_size, 1))
    came = lax.all_to_all(
        idents, ("dp", "expert", "mp"), split_axis=0, concat_axis=0, tiled=True
    )
    lie = [
        (source(copy_index, d, dp_size) * expert_size + source(expert_index, s, expert_size)) * mp_size
        + source(mp_index, t, mp_size)
        for part in (range(half), range(half, expert_size))
        for d in range(dp_size)
        for s in part
        for t in range(mp_size)
    ]
    device_count = dp_size * group_size
    pick = jnp.stack(lie)[:, None] == jnp.arange(device_count, dtype=jnp.int32)[None, :]
    ordered = jnp.sum(jnp.where(pick[:, :, None], came[None, :, :], 0), axis=1).reshape(-1)

    if dp_size == 4:
        near_1, far_2 = over_dp(near, 1, 4), over_dp(far, 2, 4)
        near_2, far_1 = over_dp(near, 2, 4), over_dp(far, 1, 4)
        nears = [near, near_1, near_2, over_dp(near_1, 2, 4)]
        fars = [far, far_1, far_2, over_dp(far_2, 1, 4)]
    else:
        nears = [near] + [over_dp(near, step, dp_size) for step in range(1, dp_size)]
        fars = [far] + [over_dp(far, step, dp_size) for step in range(1, dp_size)]
    pieces = nears + fars
    copied = copy_base(
        base_weights, (far, nears[1]), block * 4, copied, start=1, total=3
    ).reshape(base_weights.shape)

    slots = dp_size * slot_total
    block_total = exp_dev * row_blocks * col_blocks
    kept = min(slots, block_total)
    return pl.pallas_call(
        functools.partial(
            add_blocks, pieces=len(pieces), slots=slots, row_blocks=row_blocks,
            col_blocks=col_blocks, block=block, exp_dev=exp_dev,
        ),
        out_shape=jax.ShapeDtypeStruct(base_weights.shape, base_weights.dtype),
        in_specs=[pl.BlockSpec(memory_space=pltpu.SMEM)]
        + [pl.BlockSpec(memory_space=pltpu.VMEM)] * len(pieces)
        + [pl.BlockSpec(memory_space=pl.ANY)],
        out_specs=pl.BlockSpec(memory_space=pl.ANY),
        scratch_shapes=[
            pltpu.VMEM((kept, block, block), jnp.float32),
            pltpu.VMEM((kept, block, block), jnp.bfloat16),
            pltpu.SMEM((block_total,), jnp.int32),
            pltpu.SMEM((block_total,), jnp.int32),
            pltpu.SemaphoreType.DMA((kept,)),
            pltpu.SemaphoreType.DMA((kept,)),
        ],
        input_output_aliases={len(pieces) + 1: 0},
    )(ordered, *pieces, copied)


def solution(mesh):
    in_specs = (
        P("expert", None, "mp"),
        P(("dp", "expert", "mp"), None, None),
        P(("dp", "expert", "mp")),
        P(("dp", "expert", "mp")),
        P(),
    )
    out_specs = P("expert", None, "mp")
    return jax.shard_map(body, mesh=mesh, in_specs=in_specs, out_specs=out_specs, check_vma=False)
```
